32 devices in a mesh: dp: 8 (over y, x, core), tensor: 4 (over z).
Axes of the slice: x: 2, y: 2, z: 4, core: 2. Of those that a mesh axis runs over, the one named last changes fastest.
Arguments:
- tokens: bfloat16 [8192, 2048], P(('dp', 'tensor')), may hold values from -40 to 40
- ln_gain: bfloat16 [2048], P('dp'), may hold values from 0.5 to 1.5
- ln_bias: bfloat16 [2048], P('dp'), may hold values from -4 to 4
- w_qkv: bfloat16 [2048, 3, 2048], P('dp', None, 'tensor'), may hold values from -3 to 3
- qkv_bias: bfloat16 [3, 32, 64], P(None, 'tensor', 'dp'), may hold values from -0.3125 to 0.3125
- w_dense: bfloat16 [2048, 2048], P('tensor', 'dp'), may hold values from -4 to 4
- dense_bias: bfloat16 [2048], P('dp'), may hold values from -4 to 4
- w_fc1: bfloat16 [2048, 8192], P('dp', 'tensor'), may hold values from -0.125 to 0.125
- fc1_bias: bfloat16 [32, 256], P('tensor', 'dp'), may hold values from -6 to 6
- w_fc2: bfloat16 [8192, 2048], P('tensor', 'dp'), may hold values from -0.0625 to 0.0625
- fc2_bias: bfloat16 [2048], P('dp'), may hold values from -4 to 4
- cotangent: bfloat16 [8192, 2048], P(('dp', 'tensor')), may hold values from -6 to 6
Outputs:
- output: float32 [8192, 2048], P(('dp', 'tensor'))
- grad_tokens: float32 [8192, 2048], P(('dp', 'tensor'))
- grad_ln_gain: float32 [2048], P('dp')
- grad_ln_bias: float32 [2048], P('dp')
- grad_w_qkv: float32 [2048, 3, 2048], P('dp', None, 'tensor')
- grad_qkv_bias: float32 [3, 32, 64], P(None, 'tensor', 'dp')
- grad_w_dense: float32 [2048, 2048], P('tensor', 'dp')
- grad_dense_bias: float32 [2048], P('dp')
- grad_w_fc1: float32 [2048, 8192], P('dp', 'tensor')
- grad_fc1_bias: float32 [32, 256], P('tensor', 'dp')
- grad_w_fc2: float32 [8192, 2048], P('tensor', 'dp')
- grad_fc2_bias: float32 [2048], P('dp')
The draws below stay inside these ranges and needn't reach their ends.
All inputs are finite; a program needn't handle non-finite values.
Results may differ from the reference program's by a relative error of at most 0.0046.
Values may be sent and summed in bfloat16 or wider, within the bound.
A program may use at most 256 MiB of HBM per device.

```python
import jax
import jax.numpy as jnp
from jax import lax

D = 2048
H = 32
HD = 64
ROT = 32
FF = 8192
LENGTH = 1024
TOKENS = 8192


def draw_tokens(key, part):
    base_key = jax.random.fold_in(key, 101)
    noise_key, row_key, col_key = jax.random.split(base_key, 3)
    row_scale = jnp.exp(jax.random.uniform(row_key, (TOKENS, 1), jnp.float32, jnp.log(0.5), jnp.log(5.0)))
    col_scale = jnp.exp(jax.random.uniform(col_key, (1, D), jnp.float32, jnp.log(0.5), jnp.log(2.0)))
    base_vals = jax.random.truncated_normal(noise_key, -4.0, 4.0, (TOKENS, D), jnp.float32)
    return (base_vals * row_scale * col_scale).astype(jnp.bfloat16)


def draw_w_qkv(key, part):
    base_key = jax.random.fold_in(key, 202)
    noise_key = jax.random.fold_in(base_key, 0)
    base_vals = jax.random.truncated_normal(noise_key, -5.0, 5.0, (D, 3, D), jnp.float32) * (8.0 * D) ** (-0.5)
    return jnp.clip(base_vals, -3.0, 3.0).astype(jnp.bfloat16)


def with_spikes(values, key, source, target, parts, factor):
    def block_of(axis_at):
        return (jnp.arange(values.shape[axis_at]) // (values.shape[axis_at] // parts)).reshape((-1,) + (1,) * (values.ndim - 1 - axis_at))

    near = jax.random.permutation(key, parts)[block_of(target)]
    other_side = (block_of(target) + parts // 2) % parts
    return jnp.where((block_of(source) == near) | (block_of(source) == other_side), factor * values, values)


def block_levels(rng, dims, pieces, smallest, top_value):
    def one(dim, shards_of):
        steps = jax.random.uniform(jax.random.fold_in(jax.random.fold_in(rng, 6), dim), (shards_of,), jnp.float32, smallest / len(pieces), top_value / len(pieces))
        return jnp.repeat(jnp.exp(steps), dims[dim] // shards_of).reshape((-1,) + (1,) * (len(dims) - dim - 1))

    loudness = one(*pieces[0])
    for cut in pieces[1:]:
        loudness = loudness * one(*cut)
    return loudness


def gaussian(own_key, shape, spread, most, cuts=(), held_as=jnp.bfloat16):
    drawn = jax.random.normal(own_key, shape, jnp.float32) * spread
    if len(cuts) > 0:
        drawn = block_levels(own_key, shape, cuts, -0.22, 0.18) * drawn
    return jnp.clip(drawn, min=-most, max=most).astype(held_as)


def bell_draw_with(key, shape, width, bound, pieces, heavy, kind=jnp.bfloat16):
    values = width * jax.random.normal(key, shape, jnp.float32)
    if pieces:
        values = values * block_levels(key, shape, pieces, -0.22, 0.18)
    return jnp.clip(with_spikes(values, jax.random.fold_in(key, 3), *heavy), -bound, bound).astype(kind)


def setup_inputs(seed: int = 0) -> dict:
    arg_keys = jax.random.split(jax.random.key(seed), 13)
    return {
        "tokens": draw_tokens(jax.random.fold_in(arg_keys[12], 71), 0),
        "ln_gain": jnp.clip(1.0 + 0.1 * jax.random.normal(arg_keys[1], (D,), jnp.float32), 0.5, 1.5).astype(jnp.bfloat16),
        "ln_bias": gaussian(arg_keys[2], (D,), 0.3, 4.0, ((0, 8),)),
        "w_qkv": draw_w_qkv(jax.random.fold_in(arg_keys[12], 71), 0),
        "qkv_bias": gaussian(arg_keys[4], (3, H, HD), 0.02, 0.3125, ((1, 4), (2, 8))),
        "w_dense": gaussian(arg_keys[5], (D, D), (max(D // LENGTH, 1)) ** -0.5, 4.0, ((0, 4), (1, 8))),
        "dense_bias": gaussian(arg_keys[6], (D,), 0.3, 4.0, ((0, 8),)),
        "w_fc1": gaussian(arg_keys[7], (D, FF), D ** -0.5, 0.125, ((0, 8), (1, 4))),
        "fc1_bias": gaussian(arg_keys[8], (H, FF // H), 0.5, 6.0, ((0, 4), (1, 8))),
        "w_fc2": gaussian(arg_keys[9], (FF, D), FF ** -0.5, 0.0625, ((0, 4), (1, 8))),
        "fc2_bias": gaussian(arg_keys[10], (D,), 0.3, 4.0, ((0, 8),)),
        "cotangent": bell_draw_with(arg_keys[11], (TOKENS, D), 1.0, 6.0, ((0, 32),), (0, 1, 32, 2.75)),
    }


EPSILON = 1e-05
MASKED = -1e+30
GELU_C = 0.7978845608028654

def rotary_tables():
    half_rot = ROT // 2
    frequency = 10000.0 ** (-(jnp.arange(half_rot, dtype=jnp.float32) * 2.0 / ROT))
    angles = jnp.arange(LENGTH, dtype=jnp.float32)[:, None] * frequency[None, :]
    return (jnp.cos(angles), jnp.sin(angles))

def rotate(source, cosine, sine_part, direction):
    half_rot = ROT // 2
    first_half = source[..., :half_rot]
    second_half = source[..., half_rot:ROT]
    cos_wide = cosine[:, None, :]
    sin_wide = sine_part[:, None, :] * direction
    return jnp.concatenate([first_half * cos_wide - second_half * sin_wide, second_half * cos_wide + first_half * sin_wide, source[..., ROT:]], axis=-1)

def gelu_pair(pre_act):
    tanh_val = jnp.tanh(GELU_C * (pre_act + 0.044715 * pre_act * pre_act * pre_act))
    result = 0.5 * pre_act * (1.0 + tanh_val)
    slope = 0.5 * (1.0 + tanh_val) + 0.5 * pre_act * (1.0 - tanh_val * tanh_val) * GELU_C * (1.0 + 3.0 * 0.044715 * pre_act * pre_act)
    return (result, slope)

def masked_scores(query_blk, key_bf, start_row, block_rows):
    scores = jnp.einsum('qhd,khd->hqk', query_blk.astype(jnp.float32), key_bf.astype(jnp.float32)) * HD ** (-0.5)
    query_pos = start_row + jnp.arange(block_rows, dtype=jnp.int32)
    key_pos = jnp.arange(key_bf.shape[0], dtype=jnp.int32)
    allowed = key_pos[None, :] <= query_pos[:, None]
    return jnp.where(allowed[None], scores, MASKED)

def attend_forward(query_bf, key_bf, value_bf):
    length = query_bf.shape[0]
    block_rows = min(512, length)

    def one_block(block_index):
        start_row = (block_index * block_rows).astype(jnp.int32)
        query_blk = lax.dynamic_slice_in_dim(query_bf, start_row, block_rows, 0)
        scores = masked_scores(query_blk, key_bf, start_row, block_rows)
        row_max = lax.optimization_barrier(jnp.max(scores, axis=-1, keepdims=True))
        log_total = row_max[..., 0] + jnp.log(lax.optimization_barrier(jnp.sum(jnp.exp(scores - row_max), axis=-1)))
        attn_probs = jnp.exp(scores - log_total[..., None]).astype(jnp.bfloat16)
        block_out = jnp.einsum('hqk,khd->qhd', attn_probs.astype(jnp.float32), value_bf.astype(jnp.float32))
        return (block_out, log_total)
    block_outs, totals = lax.map(one_block, jnp.arange(length // block_rows, dtype=jnp.int32))
    heads = block_outs.shape[2]
    return (block_outs.reshape(length, heads, HD), jnp.transpose(totals, (1, 0, 2)).reshape(heads, length))

def attend_backward(query_bf, key_bf, value_bf, grad_out_bf, log_total, delta_row):
    length = query_bf.shape[0]
    block_rows = min(512, length)

    def one_block(running, block_index):
        grad_key, grad_value = running
        start_row = (block_index * block_rows).astype(jnp.int32)
        query_blk = lax.dynamic_slice_in_dim(query_bf, start_row, block_rows, 0)
        grad_blk = lax.dynamic_slice_in_dim(grad_out_bf, start_row, block_rows, 0)
        total_blk = lax.dynamic_slice_in_dim(log_total, start_row, block_rows, 1)
        delta_blk = lax.dynamic_slice_in_dim(delta_row, start_row, block_rows, 1)
        scores = masked_scores(query_blk, key_bf, start_row, block_rows)
        attn_probs = jnp.exp(scores - total_blk[..., None])
        probs_bf = attn_probs.astype(jnp.bfloat16)
        grad_value = grad_value + jnp.einsum('hqk,qhd->khd', probs_bf.astype(jnp.float32), grad_blk.astype(jnp.float32))
        grad_probs = jnp.einsum('qhd,khd->hqk', grad_blk.astype(jnp.float32), value_bf.astype(jnp.float32))
        grad_scores = (attn_probs * (grad_probs - delta_blk[..., None]) * HD ** (-0.5)).astype(jnp.bfloat16)
        grad_query_blk = jnp.einsum('hqk,khd->qhd', grad_scores.astype(jnp.float32), key_bf.astype(jnp.float32))
        grad_key = grad_key + jnp.einsum('hqk,qhd->khd', grad_scores.astype(jnp.float32), query_blk.astype(jnp.float32))
        return ((grad_key, grad_value), grad_query_blk)
    zero_grad = jnp.zeros(key_bf.shape, jnp.float32)
    (grad_key, grad_value), grad_query = lax.scan(one_block, (zero_grad, zero_grad), jnp.arange(length // block_rows, dtype=jnp.int32))
    return (grad_query.reshape(key_bf.shape), grad_key, grad_value)

def layer(x_seq, cot_seq, params):
    ln_gain, ln_bias, w_qkv, qkv_bias, w_dense, dense_bias, w_fc1, fc1_bias, w_fc2, fc2_bias = params
    cosine, sine_part = rotary_tables()
    x_float = x_seq.astype(jnp.float32)
    centered = x_float - lax.optimization_barrier(jnp.mean(x_float, axis=-1, keepdims=True))
    inv_std = lax.rsqrt(lax.optimization_barrier(jnp.mean(centered * centered, axis=-1, keepdims=True)) + EPSILON)
    normed = centered * inv_std
    gain_float = ln_gain.astype(jnp.float32)
    normed_bf = (normed * gain_float + ln_bias.astype(jnp.float32)).astype(jnp.bfloat16)
    qkv_matrix = w_qkv.reshape(D, 3 * D)
    qkv_all = (jnp.dot(normed_bf, qkv_matrix, preferred_element_type=jnp.float32) + qkv_bias.reshape(3 * D).astype(jnp.float32)).reshape(LENGTH, 3, H, HD)
    query_bf = rotate(qkv_all[:, 0], cosine, sine_part, 1.0).astype(jnp.bfloat16)
    key_bf = rotate(qkv_all[:, 1], cosine, sine_part, 1.0).astype(jnp.bfloat16)
    value_bf = qkv_all[:, 2].astype(jnp.bfloat16)
    attn_out, log_total = attend_forward(query_bf, key_bf, value_bf)
    attn_bf = attn_out.astype(jnp.bfloat16).reshape(LENGTH, D)
    fc_pre = jnp.dot(normed_bf, w_fc1, preferred_element_type=jnp.float32) + fc1_bias.reshape(FF).astype(jnp.float32)
    gelu_val, gelu_slope = gelu_pair(fc_pre)
    gelu_bf = gelu_val.astype(jnp.bfloat16)
    output = x_float + jnp.dot(attn_bf, w_dense, preferred_element_type=jnp.float32) + jnp.dot(gelu_bf, w_fc2, preferred_element_type=jnp.float32) + dense_bias.astype(jnp.float32) + fc2_bias.astype(jnp.float32)
    cot_float = cot_seq.astype(jnp.float32)
    grad_out_bias = lax.optimization_barrier(jnp.sum(cot_float, axis=0))
    grad_fc2 = jnp.dot(gelu_bf.T, cot_seq, preferred_element_type=jnp.float32)
    grad_dense = jnp.dot(attn_bf.T, cot_seq, preferred_element_type=jnp.float32)
    grad_pre = jnp.dot(cot_seq, w_fc2.T, preferred_element_type=jnp.float32) * gelu_slope
    grad_fc1_bias = lax.optimization_barrier(jnp.sum(grad_pre, axis=0))
    grad_pre_bf = grad_pre.astype(jnp.bfloat16)
    grad_fc1 = jnp.dot(normed_bf.T, grad_pre_bf, preferred_element_type=jnp.float32)
    grad_attn_bf = jnp.dot(cot_seq, w_dense.T, preferred_element_type=jnp.float32).astype(jnp.bfloat16)
    grad_heads = grad_attn_bf.reshape(LENGTH, H, HD)
    delta_row = lax.optimization_barrier(jnp.sum(grad_heads.astype(jnp.float32) * attn_bf.reshape(LENGTH, H, HD).astype(jnp.float32), axis=-1)).T
    grad_query, grad_key, grad_value = attend_backward(query_bf, key_bf, value_bf, grad_heads, log_total, delta_row)
    grad_query = rotate(grad_query, cosine, sine_part, -1.0)
    grad_key = rotate(grad_key, cosine, sine_part, -1.0)
    grad_qkv = jnp.stack([grad_query, grad_key, grad_value], axis=1)
    grad_qkv_bias = lax.optimization_barrier(jnp.sum(grad_qkv, axis=0))
    grad_qkv_bf = grad_qkv.reshape(LENGTH, 3 * D).astype(jnp.bfloat16)
    grad_qkv_w = jnp.dot(normed_bf.T, grad_qkv_bf, preferred_element_type=jnp.float32).reshape(D, 3, D)
    grad_normed = jnp.dot(grad_qkv_bf, qkv_matrix.T, preferred_element_type=jnp.float32) + jnp.dot(grad_pre_bf, w_fc1.T, preferred_element_type=jnp.float32)
    grad_gain = lax.optimization_barrier(jnp.sum(grad_normed * normed, axis=0))
    grad_shift = lax.optimization_barrier(jnp.sum(grad_normed, axis=0))
    grad_hat = grad_normed * gain_float
    grad_input = cot_float + inv_std * (grad_hat - lax.optimization_barrier(jnp.mean(grad_hat, axis=-1, keepdims=True)) - normed * lax.optimization_barrier(jnp.mean(grad_hat * normed, axis=-1, keepdims=True)))
    grads = (grad_gain, grad_shift, grad_qkv_w, grad_qkv_bias, grad_dense, grad_out_bias, grad_fc1, grad_fc1_bias.reshape(H, FF // H), grad_fc2)
    return (output, grad_input, grads)

def reference(tokens, ln_gain, ln_bias, w_qkv, qkv_bias, w_dense, dense_bias, w_fc1, fc1_bias, w_fc2, fc2_bias, cotangent):
    params = (ln_gain, ln_bias, w_qkv, qkv_bias, w_dense, dense_bias, w_fc1, fc1_bias, w_fc2, fc2_bias)
    count_seqs = TOKENS // LENGTH
    x_all = tokens.reshape(count_seqs, LENGTH, D)
    cot_all = cotangent.reshape(count_seqs, LENGTH, D)
    start_grads = (jnp.zeros((D,), jnp.float32), jnp.zeros((D,), jnp.float32), jnp.zeros((D, 3, D), jnp.float32), jnp.zeros((3, H, HD), jnp.float32), jnp.zeros((D, D), jnp.float32), jnp.zeros((D,), jnp.float32), jnp.zeros((D, FF), jnp.float32), jnp.zeros((H, FF // H), jnp.float32), jnp.zeros((FF, D), jnp.float32))

    def per_seq(running, pair):
        output, grad_input, grads = layer(pair[0], pair[1], params)
        return (jax.tree.map(lambda left, right: left + right, running, grads), (output, grad_input))
    grads, (outputs, grad_inputs) = lax.scan(per_seq, start_grads, (x_all, cot_all))
    grad_gain, grad_shift, grad_qkv_w, grad_qkv_bias, grad_dense, grad_out_bias, grad_fc1, grad_fc1_bias, grad_fc2 = grads
    return (outputs.reshape(TOKENS, D), grad_inputs.reshape(TOKENS, D), grad_gain, grad_shift, grad_qkv_w, grad_qkv_bias, grad_dense, grad_out_bias, grad_fc1, grad_fc1_bias, grad_fc2, grad_out_bias)
```

```python
import functools

import jax
import jax.numpy as jnp
from jax import lax
from jax.experimental import pallas as pl
from jax.experimental.pallas import tpu as pltpu
from jax.sharding import PartitionSpec as P

HD = 64
ROT = 32
LENGTH = 1024
QB = 256
EPSILON = 1e-05
MASKED = -1e30
GELU_C = 0.7978845608028654
BF = jnp.bfloat16
F32 = jnp.float32
ROWS = (((0,), (0,)), ((), ()))
COLS = (((1,), (1,)), ((), ()))
MIB = 1024 * 1024


def dot(left, right):
    return lax.dot_general(left, right, (((1,), (0,)), ((), ())), preferred_element_type=F32)


def contract(left, right, dims):
    return lax.dot_general(left, right, dims, preferred_element_type=F32)


def rotary_tables(length):
    half = ROT // 2
    frequency = 10000.0 ** (-(jnp.arange(half, dtype=F32) * 2.0 / ROT))
    angles = jnp.arange(length, dtype=F32)[:, None] * frequency[None, :]
    cos, sin = jnp.cos(angles), jnp.sin(angles)
    none = jnp.zeros((length, half), F32)
    rest = jnp.zeros((length, HD - ROT), F32)
    wide = jnp.concatenate([cos, cos, rest + 1.0] * 2, axis=1)
    up = jnp.concatenate([-sin, none, rest] * 2, axis=1)
    down = jnp.concatenate([none, sin, rest] * 2, axis=1)
    return wide, up, down


def turn(x, wide, up, down):
    return x * wide + pltpu.roll(x, 128 - ROT // 2, 1) * up + pltpu.roll(x, ROT // 2, 1) * down


def causal_scores(key, query_t, ext):
    scores = dot(key[:ext], query_t)
    last = scores[ext - QB :]
    row = lax.broadcasted_iota(jnp.int32, last.shape, 0)
    col = lax.broadcasted_iota(jnp.int32, last.shape, 1)
    last = jnp.where(row <= col, last, MASKED)
    return last if ext == QB else jnp.concatenate([scores[: ext - QB], last], axis=0)


def forward_kernel(q_ref, k_ref, v_ref, bias_ref, wide_ref, up_ref, down_ref, o_ref, qo_ref, ko_ref, vo_ref, lse_ref):
    tables = wide_ref[...], up_ref[...], down_ref[...]
    length = q_ref.shape[0]
    query = turn(q_ref[...] + bias_ref[0], *tables).astype(BF) * jnp.asarray(HD**-0.5, BF)
    key = turn(k_ref[...] + bias_ref[1], *tables).astype(BF)
    value = (v_ref[...] + bias_ref[2]).astype(BF)
    qo_ref[...], ko_ref[...], vo_ref[...] = query, key, value
    query_t, value_t = query.T, value.T
    row = lax.broadcasted_iota(jnp.int32, (128, QB), 0)
    for lo in range(0, length, QB):
        ext = lo + QB
        block = query_t[:, lo:ext]
        parts = []
        for head in range(2):
            mine = (row < HD) if head == 0 else (row >= HD)
            scores = causal_scores(key, jnp.where(mine, block, jnp.zeros_like(block)), ext)
            top = jnp.max(scores, axis=0, keepdims=True)
            weights = jnp.exp(scores - top)
            total = jnp.sum(weights, axis=0, keepdims=True)
            lse_ref[0, head : head + 1, lo:ext] = top + jnp.log(total)
            probs = (weights * (1.0 / total)).astype(BF)
            parts.append(dot(value_t[head * HD : (head + 1) * HD, :ext], probs))
        o_ref[lo:ext, :] = jnp.concatenate(parts, axis=0).T.astype(BF)


def attention_forward(qkv, bias, tables):
    length, width = qkv.shape
    inner = width // 3
    pairs = inner // 128

    def columns(offset):
        return pl.BlockSpec((length, 128), lambda g: (0, g + offset))

    table = pl.BlockSpec((length, 128), lambda g: (0, 0))
    out = jax.ShapeDtypeStruct((length, inner), BF)
    return pl.pallas_call(
        forward_kernel,
        grid=(pairs,),
        in_specs=[columns(0), columns(pairs), columns(2 * pairs), pl.BlockSpec((3, 1, 128), lambda g: (0, 0, g))]
        + [table] * 3,
        out_specs=[columns(0)] * 4 + [pl.BlockSpec((1, 2, length), lambda g: (g, 0, 0))],
        out_shape=[out] * 4 + [jax.ShapeDtypeStruct((pairs, 2, length), F32)],
        compiler_params=pltpu.CompilerParams(vmem_limit_bytes=56 * MIB),
        cost_estimate=pl.CostEstimate(
            flops=16 * length * length * inner, bytes_accessed=length * width * 8, transcendentals=0
        ),
        name="attention_forward",
    )(qkv, qkv, qkv, bias, *tables)


def backward_kernel(
    q_ref, k_ref, v_ref, o_ref, do_ref, lse_ref, wide_ref, up_ref, down_ref, dq_ref, dk_ref, dv_ref, db_ref, aq, ak, av
):
    length = q_ref.shape[0]
    query, key, value, grad = q_ref[...], k_ref[...], v_ref[...], do_ref[...]
    query_t, key_t, grad_t = query.T, key.T, grad.T
    product = grad_t.astype(F32) * o_ref[...].T.astype(F32)
    row = lax.broadcasted_iota(jnp.int32, (128, QB), 0)
    lane = lax.broadcasted_iota(jnp.int32, (QB, 128), 1)
    flat, tall = jnp.zeros((128, QB), BF), jnp.zeros((QB, 128), BF)
    for lo in range(0, length, QB):
        ext = lo + QB
        parts = []
        sum_k = sum_v = None
        for head in range(2):
            rows_in = (row < HD) if head == 0 else (row >= HD)
            lanes_in = (lane < HD) if head == 0 else (lane >= HD)
            scores = causal_scores(key, jnp.where(rows_in, query_t[:, lo:ext], flat), ext)
            probs = jnp.exp(scores - lse_ref[0, head : head + 1, lo:ext])
            grad_v = dot(probs.astype(BF), jnp.where(lanes_in, grad[lo:ext], tall))
            grad_p = dot(value[:ext], jnp.where(rows_in, grad_t[:, lo:ext], flat))
            delta = jnp.sum(product[head * HD : (head + 1) * HD, lo:ext], axis=0, keepdims=True)
            grad_s = (probs * (grad_p - delta)).astype(BF)
            grad_k = dot(grad_s, jnp.where(lanes_in, query[lo:ext], tall))
            sum_k = grad_k if sum_k is None else sum_k + grad_k
            sum_v = grad_v if sum_v is None else sum_v + grad_v
            parts.append(dot(key_t[head * HD : (head + 1) * HD, :ext], grad_s))
        aq[lo:ext, :] = jnp.concatenate(parts, axis=0).T * (HD**-0.5)
        if lo:
            ak[:lo, :] += sum_k[:lo]
            av[:lo, :] += sum_v[:lo]
        ak[lo:ext, :] = sum_k[lo:]
        av[lo:ext, :] = sum_v[lo:]
    tables = wide_ref[...], -up_ref[...], -down_ref[...]
    grad_q, grad_k, grad_v = turn(aq[...], *tables), turn(ak[...], *tables), av[...]
    for index, (total, ref) in enumerate(((grad_q, dq_ref), (grad_k, dk_ref), (grad_v, dv_ref))):
        ref[...] = total.astype(BF)
        db_ref[index] = jnp.sum(total, axis=0, keepdims=True)


def attention_backward(query, key, value, out, grad, lse, tables):
    length, inner = query.shape
    pairs = inner // 128
    columns = pl.BlockSpec((length, 128), lambda g: (0, g))
    table = pl.BlockSpec((length, 128), lambda g: (0, 0))
    shape = jax.ShapeDtypeStruct((length, inner), BF)
    return pl.pallas_call(
        backward_kernel,
        grid=(pairs,),
        in_specs=[columns] * 5 + [pl.BlockSpec((1, 2, length), lambda g: (g, 0, 0))] + [table] * 3,
        out_specs=[columns] * 3 + [pl.BlockSpec((3, 1, 128), lambda g: (0, 0, g))],
        out_shape=[shape] * 3 + [jax.ShapeDtypeStruct((3, 1, inner), F32)],
        scratch_shapes=[pltpu.VMEM((length, 128), F32)] * 3,
        compiler_params=pltpu.CompilerParams(vmem_limit_bytes=56 * MIB),
        cost_estimate=pl.CostEstimate(
            flops=20 * length * length * inner, bytes_accessed=length * inner * 20, transcendentals=0
        ),
        name="attention_backward",
    )(query, key, value, out, grad, lse, *tables)


class Cube:
    def __init__(self, size):
        self.size = size
        self.bits = size.bit_length() - 1
        self.high = list(range(1, self.bits))
        self.order = sorted(range(size), key=self.place)

    def place(self, mask):
        return (mask % 2) * (self.size // 2) + mask // 2

    def swap(self, value, bit):
        return lax.ppermute(value, "dp", [(i, i ^ (1 << bit)) for i in range(self.size)])

    def to_own(self, value, axis):
        own = lax.axis_index("dp")
        width = value.shape[axis] // self.size
        return jnp.concatenate(
            [lax.dynamic_slice_in_dim(value, (own ^ mask) * width, width, axis) for mask in self.order], axis
        )

    def from_own(self, value, axis):
        own = lax.axis_index("dp")
        width = value.shape[axis] // self.size
        return jnp.concatenate(
            [
                lax.dynamic_slice_in_dim(value, self.place(own ^ block) * width, width, axis)
                for block in range(self.size)
            ],
            axis,
        )

    def gather(self, shard, bits, axis):
        held, masks = shard[None], [0]
        pieces = {}
        for index, bit in enumerate([*bits, 0]):
            other = self.swap(held, bit)
            fresh = [mask | (1 << bit) for mask in masks]
            if index == len(bits):
                pieces = {mask: held[i] for i, mask in enumerate(masks)}
                pieces |= {mask: other[i] for i, mask in enumerate(fresh)}
            else:
                held, masks = jnp.concatenate([held, other]), masks + fresh
        return jnp.concatenate([pieces[mask] for mask in self.order], axis)

    def scatter(self, partial, bits, axis):
        half = self.size // 2
        received = self.swap(partial(half, self.size).astype(BF), 0)
        kept = partial(0, half) + received.astype(F32)
        masks = self.order[:half]
        for bit in bits:
            width = kept.shape[axis] // len(masks)

            def pick(flag):
                chosen = [i for i, mask in enumerate(masks) if mask >> bit & 1 == flag]
                return jnp.concatenate([lax.slice_in_dim(kept, i * width, (i + 1) * width, axis=axis) for i in chosen], axis)

            received = self.swap(pick(1).astype(BF), bit)
            kept = pick(0) + received.astype(F32)
            masks = [mask for mask in masks if not mask >> bit & 1]
        return kept


def gelu_pair(pre_act):
    tanh_val = jnp.tanh(GELU_C * (pre_act + 0.044715 * pre_act * pre_act * pre_act))
    result = 0.5 * pre_act * (1.0 + tanh_val)
    slope = 0.5 * (1.0 + tanh_val) + 0.5 * pre_act * (1.0 - tanh_val * tanh_val) * GELU_C * (
        1.0 + 3.0 * 0.044715 * pre_act * pre_act
    )
    return (result, slope)


def standardize(rows):
    x = rows.astype(F32)
    centered = x - jnp.mean(x, axis=-1, keepdims=True)
    inv_std = lax.rsqrt(jnp.mean(centered * centered, axis=-1, keepdims=True) + EPSILON)
    return centered * inv_std, inv_std


def body(
    size,
    tokens,
    ln_gain,
    ln_bias,
    w_qkv,
    qkv_bias,
    w_dense,
    dense_bias,
    w_fc1,
    fc1_bias,
    w_fc2,
    fc2_bias,
    cotangent,
):
    cube = Cube(size)
    up, down = cube.high, cube.high[::-1]
    depth, _, inner = w_qkv.shape
    hidden = w_fc1.shape[1]
    width = tokens.shape[1]
    heads = inner // HD
    own = lax.axis_index("dp")

    rows_all = lax.all_gather(cube.to_own(tokens, 1), "tensor", axis=0, tiled=True)
    cot_all = lax.all_gather(cube.to_own(cotangent, 1), "tensor", axis=0, tiled=True)

    qkv_w = cube.gather(w_qkv.reshape(depth, 3 * inner), down, 0)
    fc1_w = cube.gather(w_fc1, up, 0)
    dense_w = cube.gather(w_dense, up, 1)
    fc2_w = cube.gather(w_fc2, down, 1)

    small = jnp.concatenate(
        [ln_gain, ln_bias, dense_bias, fc2_bias, qkv_bias.reshape(-1), fc1_bias.reshape(-1)]
    )
    small = lax.all_gather(small, "dp", axis=0)
    gain, shift = (small[:, i * depth : (i + 1) * depth].reshape(-1) for i in range(2))
    out_bias = small[:, 2 * depth : 3 * depth].astype(F32) + small[:, 3 * depth : 4 * depth].astype(F32)
    cut = 4 * depth + qkv_bias.size
    bias_qkv = small[:, 4 * depth : cut].reshape(size, 3, heads, -1).transpose(1, 2, 0, 3).reshape(3, 1, inner)
    bias_fc1 = small[:, cut:].reshape(size, heads, -1).transpose(1, 0, 2).reshape(hidden)
    own_gain, own_shift = cube.to_own(gain.astype(F32), 0), cube.to_own(shift.astype(F32), 0)

    tables = rotary_tables(LENGTH)
    normed_bf = (standardize(rows_all)[0] * own_gain + own_shift).astype(BF)
    qkv = dot(normed_bf, qkv_w)
    attn_bf, query, key, value, lse = attention_forward(qkv, bias_qkv.astype(F32), tables)
    fc_pre = dot(normed_bf, fc1_w) + bias_fc1.astype(F32)
    gelu, slope = gelu_pair(fc_pre)
    gelu_bf = gelu.astype(BF)
    branch = (dot(attn_bf, dense_w) + dot(gelu_bf, fc2_w)).astype(BF)
    branch = lax.psum_scatter(branch, "tensor", scatter_dimension=0, tiled=True)
    output = tokens.astype(F32) + cube.from_own(branch, 1).astype(F32) + out_bias.reshape(-1)

    grad_attn = contract(cot_all, dense_w, COLS).astype(BF)
    grad_q, grad_k, grad_v, grad_qkv_bias = attention_backward(query, key, value, attn_bf, grad_attn, lse, tables)
    grad_pre = contract(cot_all, fc2_w, COLS) * slope
    grad_fc1_bias = jnp.sum(grad_pre, axis=0)
    grad_pre_bf = grad_pre.astype(BF)
    grad_qkv = jnp.concatenate([grad_q, grad_k, grad_v], axis=1)
    grad_normed = contract(grad_qkv, qkv_w, COLS) + contract(grad_pre_bf, fc1_w, COLS)
    gain_part = jnp.sum(grad_normed * standardize(rows_all)[0], axis=0)
    shift_part = jnp.sum(grad_normed, axis=0)
    grad_rows = lax.psum_scatter(grad_normed.astype(BF), "tensor", scatter_dimension=0, tiled=True)

    def columns(left, right):
        return lambda lo, hi: contract(left, right[:, lo * depth : hi * depth], ROWS)

    def rows(left, right):
        return lambda lo, hi: contract(left[:, lo * depth : hi * depth], right, ROWS)

    fc2_out = cube.scatter(columns(gelu_bf, cot_all), down, 1)
    dense_out = cube.scatter(columns(attn_bf, cot_all), up, 1)
    fc1_out = cube.scatter(rows(normed_bf, grad_pre_bf), up, 0)
    qkv_out = cube.scatter(rows(normed_bf, grad_qkv), down, 0)

    cot_part = jnp.sum(cotangent.astype(F32), axis=0)
    parts = jnp.concatenate(
        [
            cube.from_own(gain_part, 0).reshape(size, depth),
            cube.from_own(shift_part, 0).reshape(size, depth),
            cot_part.reshape(size, depth),
            grad_qkv_bias.reshape(3, heads, size, -1).transpose(2, 0, 1, 3).reshape(size, -1),
            grad_fc1_bias.reshape(heads, size, -1).transpose(1, 0, 2).reshape(size, -1),
        ],
        axis=1,
    )
    sums = lax.all_gather(parts, "dp", axis=0)
    sums = jnp.sum(lax.dynamic_index_in_dim(sums, own, 1, keepdims=False), axis=0)
    wide = jnp.sum(lax.all_gather(sums[: 3 * depth], "tensor", axis=0), axis=0)
    gain_out, shift_out, bias_out = (wide[i * depth : (i + 1) * depth] for i in range(3))
    cut = 3 * depth + qkv_bias.size
    qkv_bias_out = sums[3 * depth : cut].reshape(qkv_bias.shape)
    fc1_bias_out = sums[cut:].reshape(fc1_bias.shape)

    normed, inv_std = standardize(tokens)
    grad_hat = cube.from_own(grad_rows, 1).astype(F32) * gain.astype(F32)
    grad_tokens = cotangent.astype(F32) + inv_std * (
        grad_hat
        - jnp.mean(grad_hat, axis=-1, keepdims=True)
        - normed * jnp.mean(grad_hat * normed, axis=-1, keepdims=True)
    )
    return (
        output,
        grad_tokens,
        gain_out,
        shift_out,
        qkv_out.reshape(depth, 3, inner),
        qkv_bias_out,
        dense_out,
        bias_out,
        fc1_out,
        fc1_bias_out,
        fc2_out,
        bias_out,
    )


def solution(mesh):
    in_specs = (
        P(("dp", "tensor"), None),
        P("dp"),
        P("dp"),
        P("dp", None, "tensor"),
        P(None, "tensor", "dp"),
        P("tensor", "dp"),
        P("dp"),
        P("dp", "tensor"),
        P("tensor", "dp"),
        P("tensor", "dp"),
        P("dp"),
        P(("dp", "tensor"), None),
    )
    out_specs = (
        P(("dp", "tensor"), None),
        P(("dp", "tensor"), None),
        P("dp"),
        P("dp"),
        P("dp", None, "tensor"),
        P(None, "tensor", "dp"),
        P("tensor", "dp"),
        P("dp"),
        P("dp", "tensor"),
        P("tensor", "dp"),
        P("tensor", "dp"),
        P("dp"),
    )
    step = functools.partial(body, mesh.shape["dp"])
    return jax.shard_map(step, mesh=mesh, in_specs=in_specs, out_specs=out_specs, check_vma=False)
```

```python
import functools

import jax
import jax.numpy as jnp
from jax import lax
from jax.experimental import pallas as pl
from jax.experimental.pallas import tpu as pltpu
from jax.sharding import PartitionSpec as P

HD = 64
ROT = 32
LENGTH = 1024
QB = 256
EPSILON = 1e-05
MASKED = -1e30
GELU_C = 0.7978845608028654
BF = jnp.bfloat16
F32 = jnp.float32
ROWS = (((0,), (0,)), ((), ()))
COLS = (((1,), (1,)), ((), ()))
MIB = 1024 * 1024


def dot(left, right):
    return lax.dot_general(left, right, (((1,), (0,)), ((), ())), preferred_element_type=F32)


def contract(left, right, dims):
    return lax.dot_general(left, right, dims, preferred_element_type=F32)


def rotary_tables(length):
    half = ROT // 2
    frequency = 10000.0 ** (-(jnp.arange(half, dtype=F32) * 2.0 / ROT))
    angles = jnp.arange(length, dtype=F32)[:, None] * frequency[None, :]
    cos, sin = jnp.cos(angles), jnp.sin(angles)
    none = jnp.zeros((length, half), F32)
    rest = jnp.zeros((length, HD - ROT), F32)
    wide = jnp.concatenate([cos, cos, rest + 1.0] * 2, axis=1)
    up = jnp.concatenate([-sin, none, rest] * 2, axis=1)
    down = jnp.concatenate([none, sin, rest] * 2, axis=1)
    return wide, up, down


def turn(x, wide, up, down):
    return x * wide + pltpu.roll(x, 128 - ROT // 2, 1) * up + pltpu.roll(x, ROT // 2, 1) * down


def causal_scores(key, query_t, ext):
    scores = dot(key[:ext], query_t)
    last = scores[ext - QB :]
    row = lax.broadcasted_iota(jnp.int32, last.shape, 0)
    col = lax.broadcasted_iota(jnp.int32, last.shape, 1)
    last = jnp.where(row <= col, last, MASKED)
    return last if ext == QB else jnp.concatenate([scores[: ext - QB], last], axis=0)


def forward_kernel(q_ref, k_ref, v_ref, bias_ref, wide_ref, up_ref, down_ref, o_ref, qo_ref, ko_ref, vo_ref, lse_ref):
    tables = wide_ref[...], up_ref[...], down_ref[...]
    length = q_ref.shape[0]
    query = turn(q_ref[...] + bias_ref[0], *tables).astype(BF) * jnp.asarray(HD**-0.5, BF)
    key = turn(k_ref[...] + bias_ref[1], *tables).astype(BF)
    value = (v_ref[...] + bias_ref[2]).astype(BF)
    qo_ref[...], ko_ref[...], vo_ref[...] = query, key, value
    query_t, value_t = query.T, value.T
    row = lax.broadcasted_iota(jnp.int32, (128, QB), 0)
    for lo in range(0, length, QB):
        ext = lo + QB
        block = query_t[:, lo:ext]
        parts = []
        for head in range(2):
            mine = (row < HD) if head == 0 else (row >= HD)
            scores = causal_scores(key, jnp.where(mine, block, jnp.zeros_like(block)), ext)
            top = jnp.max(scores, axis=0, keepdims=True)
            weights = jnp.exp(scores - top)
            total = jnp.sum(weights, axis=0, keepdims=True)
            lse_ref[0, head : head + 1, lo:ext] = top + jnp.log(total)
            probs = (weights * (1.0 / total)).astype(BF)
            parts.append(dot(value_t[head * HD : (head + 1) * HD, :ext], probs))
        o_ref[lo:ext, :] = jnp.concatenate(parts, axis=0).T.astype(BF)


def attention_forward(qkv, bias, tables):
    length, width = qkv.shape
    inner = width // 3
    pairs = inner // 128

    def columns(offset):
        return pl.BlockSpec((length, 128), lambda g: (0, g + offset))

    table = pl.BlockSpec((length, 128), lambda g: (0, 0))
    out = jax.ShapeDtypeStruct((length, inner), BF)
    return pl.pallas_call(
        forward_kernel,
        grid=(pairs,),
        in_specs=[columns(0), columns(pairs), columns(2 * pairs), pl.BlockSpec((3, 1, 128), lambda g: (0, 0, g))]
        + [table] * 3,
        out_specs=[columns(0)] * 4 + [pl.BlockSpec((1, 2, length), lambda g: (g, 0, 0))],
        out_shape=[out] * 4 + [jax.ShapeDtypeStruct((pairs, 2, length), F32)],
        compiler_params=pltpu.CompilerParams(vmem_limit_bytes=56 * MIB),
        cost_estimate=pl.CostEstimate(
            flops=16 * length * length * inner, bytes_accessed=length * width * 8, transcendentals=0
        ),
        name="attention_forward",
    )(qkv, qkv, qkv, bias, *tables)


def backward_kernel(
    q_ref, k_ref, v_ref, o_ref, do_ref, lse_ref, wide_ref, up_ref, down_ref, dq_ref, dk_ref, dv_ref, db_ref, aq, ak, av
):
    length = q_ref.shape[0]
    query, key, value, grad = q_ref[...], k_ref[...], v_ref[...], do_ref[...]
    query_t, key_t, grad_t = query.T, key.T, grad.T
    product = grad_t.astype(F32) * o_ref[...].T.astype(F32)
    row = lax.broadcasted_iota(jnp.int32, (128, QB), 0)
    lane = lax.broadcasted_iota(jnp.int32, (QB, 128), 1)
    flat, tall = jnp.zeros((128, QB), BF), jnp.zeros((QB, 128), BF)
    for lo in range(0, length, QB):
        ext = lo + QB
        parts = []
        sum_k = sum_v = None
        for head in range(2):
            rows_in = (row < HD) if head == 0 else (row >= HD)
            lanes_in = (lane < HD) if head == 0 else (lane >= HD)
            scores = causal_scores(key, jnp.where(rows_in, query_t[:, lo:ext], flat), ext)
            probs = jnp.exp(scores - lse_ref[0, head : head + 1, lo:ext])
            grad_v = dot(probs.astype(BF), jnp.where(lanes_in, grad[lo:ext], tall))
            grad_p = dot(value[:ext], jnp.where(rows_in, grad_t[:, lo:ext], flat))
            delta = jnp.sum(product[head * HD : (head + 1) * HD, lo:ext], axis=0, keepdims=True)
            grad_s = (probs * (grad_p - delta)).astype(BF)
            grad_k = dot(grad_s, jnp.where(lanes_in, query[lo:ext], tall))
            sum_k = grad_k if sum_k is None else sum_k + grad_k
            sum_v = grad_v if sum_v is None else sum_v + grad_v
            parts.append(dot(key_t[head * HD : (head + 1) * HD, :ext], grad_s))
        aq[lo:ext, :] = jnp.concatenate(parts, axis=0).T * (HD**-0.5)
        if lo:
            ak[:lo, :] += sum_k[:lo]
            av[:lo, :] += sum_v[:lo]
        ak[lo:ext, :] = sum_k[lo:]
        av[lo:ext, :] = sum_v[lo:]
    tables = wide_ref[...], -up_ref[...], -down_ref[...]
    grad_q, grad_k, grad_v = turn(aq[...], *tables), turn(ak[...], *tables), av[...]
    for index, (total, ref) in enumerate(((grad_q, dq_ref), (grad_k, dk_ref), (grad_v, dv_ref))):
        ref[...] = total.astype(BF)
        db_ref[index] = jnp.sum(total, axis=0, keepdims=True)


def attention_backward(query, key, value, out, grad, lse, tables):
    length, inner = query.shape
    pairs = inner // 128
    columns = pl.BlockSpec((length, 128), lambda g: (0, g))
    table = pl.BlockSpec((length, 128), lambda g: (0, 0))
    shape = jax.ShapeDtypeStruct((length, inner), BF)
    return pl.pallas_call(
        backward_kernel,
        grid=(pairs,),
        in_specs=[columns] * 5 + [pl.BlockSpec((1, 2, length), lambda g: (g, 0, 0))] + [table] * 3,
        out_specs=[columns] * 3 + [pl.BlockSpec((3, 1, 128), lambda g: (0, 0, g))],
        out_shape=[shape] * 3 + [jax.ShapeDtypeStruct((3, 1, inner), F32)],
        scratch_shapes=[pltpu.VMEM((length, 128), F32)] * 3,
        compiler_params=pltpu.CompilerParams(vmem_limit_bytes=56 * MIB),
        cost_estimate=pl.CostEstimate(
            flops=20 * length * length * inner, bytes_accessed=length * inner * 20, transcendentals=0
        ),
        name="attention_backward",
    )(query, key, value, out, grad, lse, *tables)


def call(kernel, name, grid, in_specs, out_specs, out_shape, flops, scalars=0, scratch=()):
    bytes_accessed = sum(leaf.size * leaf.dtype.itemsize for leaf in jax.tree.leaves(out_shape)) * 2
    return pl.pallas_call(
        kernel,
        grid_spec=pltpu.PrefetchScalarGridSpec(
            num_scalar_prefetch=scalars, grid=grid, in_specs=in_specs, out_specs=out_specs, scratch_shapes=scratch
        ),
        out_shape=out_shape,
        compiler_params=pltpu.CompilerParams(vmem_limit_bytes=58 * MIB),
        cost_estimate=pl.CostEstimate(flops=flops, bytes_accessed=bytes_accessed, transcendentals=0),
        name=name,
    )


def whole(shape):
    return pl.BlockSpec(shape, lambda *_: (0,) * len(shape))


def shape_of(shape, dtype):
    return jax.ShapeDtypeStruct(shape, dtype)


def take_blocks(value, index, width):
    rows, columns = value.shape
    if width % 128:
        blocks = [lax.dynamic_slice_in_dim(value, index[i] * width, width, 1) for i in range(index.shape[0])]
        return jnp.concatenate(blocks, axis=1)

    def kernel(index_ref, in_ref, out_ref):
        for i in range(columns // width):
            start = pl.multiple_of(index_ref[i] * width, width)
            out_ref[:, i * width : (i + 1) * width] = in_ref[:, pl.ds(start, width)]

    block = pl.BlockSpec((rows // 2, columns), lambda i, index: (i, 0))
    return call(kernel, "take_blocks", (2,), [block], block, shape_of(value.shape, value.dtype), 0, 1)(index, value)


def normalize(rows, gain, shift, index, width):
    count, columns = rows.shape
    tile = 256

    def kernel(index_ref, x_ref, gain_ref, shift_ref, out_ref, mean_ref, inv_ref):
        x = x_ref[...].astype(F32)
        mean = jnp.mean(x, axis=-1, keepdims=True)
        centered = x - mean
        inv_std = lax.rsqrt(jnp.mean(centered * centered, axis=-1, keepdims=True) + EPSILON)
        mean_ref[...], inv_ref[...] = mean, inv_std
        for i in range(columns // width):
            place = pl.ds(pl.multiple_of(index_ref[i] * width, width), width)
            normed = (x_ref[:, place].astype(F32) - mean) * inv_std
            out_ref[:, i * width : (i + 1) * width] = (normed * gain_ref[:, place] + shift_ref[:, place]).astype(BF)

    block = pl.BlockSpec((tile, columns), lambda i, index: (i, 0))
    column = pl.BlockSpec((tile, 1), lambda i, index: (i, 0))
    return call(
        kernel,
        "normalize",
        (count // tile,),
        [block, whole((1, columns)), whole((1, columns))],
        [block, column, column],
        [shape_of((count, columns), BF), shape_of((count, 1), F32), shape_of((count, 1), F32)],
        count * columns * 16,
        1,
    )(index, rows, gain, shift)


def stacked(near_ref, far_ref, perm, axis, *inner):
    return jnp.concatenate([ref[(i, *inner)] for ref in (near_ref, far_ref) for i in perm], axis=axis)


def project_qkv(x, weight):
    near, far, perm = weight
    rows, width = x.shape
    half, parts, depth, inner = near.shape

    def kernel(x_ref, near_ref, far_ref, out_ref):
        out_ref[...] = dot(x_ref[...], stacked(near_ref, far_ref, perm, 0, 0))

    block = pl.BlockSpec((half, 1, depth, inner), lambda i: (0, i, 0, 0))
    return call(
        kernel,
        "project_qkv",
        (parts,),
        [whole(x.shape), block, block],
        pl.BlockSpec((rows, inner), lambda i: (0, i)),
        shape_of((rows, parts * inner), F32),
        2 * rows * width * parts * inner,
    )(x, near, far)


def gelu_pair(pre_act):
    tanh_val = jnp.tanh(GELU_C * (pre_act + 0.044715 * pre_act * pre_act * pre_act))
    result = 0.5 * pre_act * (1.0 + tanh_val)
    slope = 0.5 * (1.0 + tanh_val) + 0.5 * pre_act * (1.0 - tanh_val * tanh_val) * GELU_C * (
        1.0 + 3.0 * 0.044715 * pre_act * pre_act
    )
    return (result, slope)


def project_fc1(x, weight, bias):
    near, far, perm = weight
    rows, width = x.shape
    half, depth, hidden = near.shape
    tile = 512

    def kernel(x_ref, near_ref, far_ref, bias_ref, gelu_ref, slope_ref):
        pre_act = dot(x_ref[...], stacked(near_ref, far_ref, perm, 0)) + bias_ref[...]
        gelu, slope_ref[...] = gelu_pair(pre_act)
        gelu_ref[...] = gelu.astype(BF)

    block = pl.BlockSpec((half, depth, tile), lambda i: (0, 0, i))
    column = pl.BlockSpec((rows, tile), lambda i: (0, i))
    return call(
        kernel,
        "project_fc1",
        (hidden // tile,),
        [whole(x.shape), block, block, pl.BlockSpec((1, tile), lambda i: (0, i))],
        [column, column],
        [shape_of((rows, hidden), BF), shape_of((rows, hidden), F32)],
        2 * rows * width * hidden,
    )(x, near, far, bias)


def lookups(perm):
    half = len(perm)
    near = [perm[min(i, half - 1)] for i in range(2 * half)]
    return jnp.asarray(near + [perm[max(i - half, 0)] for i in range(2 * half)], jnp.int32)


def pick_near(half, rest):
    return lambda i, *tables: (tables[-1][i], *rest)


def pick_far(half, rest):
    return lambda i, *tables: (tables[-1][2 * half + i], *rest)


def project_out(attn, gelu, dense, fc2):
    rows, inner = attn.shape
    hidden = gelu.shape[1]
    half, _, depth = fc2[0].shape
    order = lookups(fc2[2]), lookups(dense[2])

    def kernel(fc2_at, dense_at, attn_ref, gelu_ref, dense_near, dense_far, fc2_near, fc2_far, out_ref):
        def write(dense_ref, fc2_ref):
            out_ref[...] = (dot(gelu_ref[...], fc2_ref[0]) + dot(attn_ref[...], dense_ref[0])).astype(BF)

        pl.when(pl.program_id(0) < half)(lambda: write(dense_near, fc2_near))
        pl.when(pl.program_id(0) >= half)(lambda: write(dense_far, fc2_far))

    def at(table, base):
        return lambda i, *tables: (tables[table][base + i], 0, 0)

    return call(
        kernel,
        "project_out",
        (2 * half,),
        [
            whole(attn.shape),
            whole(gelu.shape),
            pl.BlockSpec((1, inner, depth), at(1, 0)),
            pl.BlockSpec((1, inner, depth), at(1, 2 * half)),
            pl.BlockSpec((1, hidden, depth), at(0, 0)),
            pl.BlockSpec((1, hidden, depth), at(0, 2 * half)),
        ],
        pl.BlockSpec((rows, depth), lambda i, *_: (0, i)),
        shape_of((rows, 2 * half * depth), BF),
        2 * rows * (inner + hidden) * 2 * half * depth,
        2,
    )(*order, attn, gelu, dense[0], dense[1], fc2[0], fc2[1])


def back_attn(cot, dense):
    near, far, perm = dense
    inner = near.shape[1]
    rows = cot.shape[0]
    tile = rows // 4

    def kernel(cot_ref, near_ref, far_ref, out_ref):
        out_ref[...] = contract(cot_ref[...], stacked(near_ref, far_ref, perm, 1), COLS).astype(BF)

    return call(
        kernel,
        "back_attn",
        (4,),
        [pl.BlockSpec((tile, cot.shape[1]), lambda i: (i, 0)), whole(near.shape), whole(far.shape)],
        pl.BlockSpec((tile, inner), lambda i: (i, 0)),
        shape_of((rows, inner), BF),
        2 * cot.size * inner,
    )(cot, near, far)


def back_fc2(cot, fc2, slope):
    near, far, perm = fc2
    half, hidden, depth = near.shape
    rows = cot.shape[0]
    tile = 512

    def kernel(cot_ref, near_ref, far_ref, slope_ref, out_ref, bias_ref):
        grad = contract(cot_ref[...], stacked(near_ref, far_ref, perm, 1), COLS) * slope_ref[...]
        out_ref[...] = grad.astype(BF)
        bias_ref[...] = jnp.sum(grad, axis=0, keepdims=True)

    block = pl.BlockSpec((half, tile, depth), lambda i: (0, i, 0))
    column = pl.BlockSpec((rows, tile), lambda i: (0, i))
    return call(
        kernel,
        "back_fc2",
        (hidden // tile,),
        [whole(cot.shape), block, block, column],
        [column, pl.BlockSpec((1, tile), lambda i: (0, i))],
        [shape_of((rows, hidden), BF), shape_of((1, hidden), F32)],
        2 * cot.size * hidden,
    )(cot, near, far, slope)


def back_rows(grads, grad_pre, qkv, fc1, rows_all, mean, inv_std, index):
    half, parts, depth, inner = qkv[0].shape
    rows, hidden = grad_pre.shape
    order = lookups(fc1[2]), lookups(qkv[2])

    def kernel(index_ref, fc1_at, qkv_at, q_ref, k_ref, v_ref, pre_ref, qkv_near, qkv_far, near, far, *refs):
        x_ref, mean_ref, inv_ref, out_ref, gain_ref, shift_ref = refs

        def write(qkv_ref, fc1_ref):
            grad = contract(pre_ref[...], fc1_ref[0], COLS)
            for part, ref in enumerate((q_ref, k_ref, v_ref)):
                grad += contract(ref[...], qkv_ref[0, part], COLS)
            out_ref[...] = grad.astype(BF)
            normed = (x_ref[...].astype(F32) - mean_ref[...]) * inv_ref[...]
            gain_ref[...] = jnp.sum(grad * normed, axis=0, keepdims=True)
            shift_ref[...] = jnp.sum(grad, axis=0, keepdims=True)

        pl.when(pl.program_id(0) < half)(lambda: write(qkv_near, near))
        pl.when(pl.program_id(0) >= half)(lambda: write(qkv_far, far))

    def at(table, base, zeros):
        return lambda i, *tables: (tables[table][base + i], *(0,) * zeros)

    row = pl.BlockSpec((1, depth), lambda i, *_: (0, i))
    return call(
        kernel,
        "back_rows",
        (2 * half,),
        [whole(grads[0].shape)] * 3
        + [
            whole(grad_pre.shape),
            pl.BlockSpec((1, parts, depth, inner), at(2, 0, 3)),
            pl.BlockSpec((1, parts, depth, inner), at(2, 2 * half, 3)),
            pl.BlockSpec((1, depth, hidden), at(1, 0, 2)),
            pl.BlockSpec((1, depth, hidden), at(1, 2 * half, 2)),
            pl.BlockSpec((rows, depth), lambda i, index, *_: (0, index[i])),
            whole(mean.shape),
            whole(mean.shape),
        ],
        [pl.BlockSpec((rows, depth), lambda i, *_: (0, i)), row, row],
        [shape_of((rows, 2 * half * depth), BF)] + [shape_of((1, 2 * half * depth), F32)] * 2,
        2 * rows * (hidden + parts * inner) * 2 * half * depth,
        3,
    )(index, *order, *grads, grad_pre, qkv[0], qkv[1], fc1[0], fc1[1], rows_all, mean, inv_std)


def finish_output(tokens, branch, bias, index, width):
    rows, columns = tokens.shape
    tile = rows // 2

    def kernel(index_ref, x_ref, branch_ref, bias_ref, out_ref):
        for i in range(columns // width):
            here = slice(i * width, (i + 1) * width)
            place = pl.ds(pl.multiple_of(index_ref[i] * width, width), width)
            out_ref[:, here] = x_ref[:, here].astype(F32) + branch_ref[:, place].astype(F32) + bias_ref[:, here]

    block = pl.BlockSpec((tile, columns), lambda i, index: (i, 0))
    return call(
        kernel,
        "finish_output",
        (2,),
        [block, block, whole((1, columns))],
        block,
        shape_of(tokens.shape, F32),
        rows * columns * 4,
        1,
    )(index, tokens, branch, bias)


def finish_tokens(tokens, cotangent, grad, gain, index, width):
    rows, columns = tokens.shape
    tile = rows // 4

    def kernel(index_ref, x_ref, cot_ref, grad_ref, gain_ref, out_ref):
        x = x_ref[...].astype(F32)
        centered = x - jnp.mean(x, axis=-1, keepdims=True)
        inv_std = lax.rsqrt(jnp.mean(centered * centered, axis=-1, keepdims=True) + EPSILON)
        normed = centered * inv_std
        places = [pl.ds(pl.multiple_of(index_ref[i] * width, width), width) for i in range(columns // width)]
        hat = jnp.concatenate([grad_ref[:, place] for place in places], axis=1).astype(F32) * gain_ref[...]
        first = jnp.mean(hat, axis=-1, keepdims=True)
        second = jnp.mean(hat * normed, axis=-1, keepdims=True)
        out_ref[...] = cot_ref[...].astype(F32) + inv_std * (hat - first - normed * second)

    block = pl.BlockSpec((tile, columns), lambda i, index: (i, 0))
    return call(
        kernel,
        "finish_tokens",
        (4,),
        [block, block, block, whole((1, columns))],
        block,
        shape_of(tokens.shape, F32),
        rows * columns * 16,
        1,
    )(index, tokens, cotangent, grad, gain)


class Cube:
    def __init__(self, size):
        self.size = size
        self.bits = size.bit_length() - 1
        self.high = list(range(1, self.bits))
        self.order = sorted(range(size), key=lambda mask: (mask % 2, mask))

    def swap(self, value, bit):
        return lax.ppermute(value, "dp", [(i, i ^ (1 << bit)) for i in range(self.size)])

    def blocks_here(self):
        return lax.axis_index("dp") ^ jnp.asarray(self.order, jnp.int32)

    def places_here(self):
        mask = lax.axis_index("dp") ^ jnp.arange(self.size, dtype=jnp.int32)
        return (mask & 1) * (self.size // 2) + (mask >> 1)

    def gather(self, shard, bits):
        held, masks = shard[None], [0]
        for bit in bits:
            held = jnp.concatenate([held, self.swap(held, bit)])
            masks = masks + [mask | (1 << bit) for mask in masks]
        return held, self.swap(held, 0), [masks.index(mask) for mask in self.order[: len(masks)]]

    def scatter(self, partial, bits, axis):
        half = self.size // 2
        received = self.swap(partial(half, self.size).astype(BF), 0)
        kept = partial(0, half) + received.astype(F32)
        masks = self.order[:half]
        for bit in bits:
            width = kept.shape[axis] // len(masks)

            def pick(flag):
                chosen = [i for i, mask in enumerate(masks) if mask >> bit & 1 == flag]
                return jnp.concatenate([lax.slice_in_dim(kept, i * width, (i + 1) * width, axis=axis) for i in chosen], axis)

            received = self.swap(pick(1).astype(BF), bit)
            kept = pick(0) + received.astype(F32)
            masks = [mask for mask in masks if not mask >> bit & 1]
        return kept


def widen(gathered, axis, width):
    near, far, perm = gathered
    if near.shape[axis] % 128 == 0:
        return gathered
    full = jnp.concatenate([part[i] for part in (near, far) for i in perm], axis - 1)
    count = full.shape[axis - 1] // width
    blocks = jnp.stack(jnp.split(full, count, axis - 1))
    return blocks[: count // 2], blocks[count // 2 :], list(range(count // 2))


def body(
    size,
    tokens,
    ln_gain,
    ln_bias,
    w_qkv,
    qkv_bias,
    w_dense,
    dense_bias,
    w_fc1,
    fc1_bias,
    w_fc2,
    fc2_bias,
    cotangent,
):
    cube = Cube(size)
    up, down = cube.high, cube.high[::-1]
    depth, _, inner = w_qkv.shape
    hidden = w_fc1.shape[1]
    width = tokens.shape[1]
    heads = inner // HD
    blocks, places = cube.blocks_here(), cube.places_here()
    if depth % 128 == 0:
        wide, enter, leave = depth, blocks, places
        rows_all = lax.all_gather(tokens, "tensor", axis=0, tiled=True)
    else:
        wide = 256
        enter = leave = jnp.arange(width // wide, dtype=jnp.int32)
        rows_all = lax.all_gather(take_blocks(tokens, blocks, depth), "tensor", axis=0, tiled=True)

    small = jnp.concatenate(
        [ln_gain, ln_bias, dense_bias, fc2_bias, qkv_bias.reshape(-1), fc1_bias.reshape(-1)]
    )
    extra = -(-small.size // depth // 16) * 16
    small_rows = jnp.pad(small, (0, extra * depth - small.size)).reshape(extra, depth)
    dense_w = cube.gather(jnp.concatenate([w_dense, small_rows]), down)
    qkv_w = cube.gather(w_qkv.transpose(1, 0, 2), up)
    fc1_w = cube.gather(w_fc1, down)
    fc2_w = cube.gather(w_fc2, up)

    cot_all = lax.all_gather(take_blocks(cotangent, blocks, depth), "tensor", axis=0, tiled=True)

    small = jnp.concatenate([part[i : i + 1, inner:] for part in dense_w[:2] for i in dense_w[2]]).reshape(size, -1)
    small = jnp.take(small, places, axis=0)
    gain, shift = (small[:, i * depth : (i + 1) * depth].astype(F32) for i in range(2))
    if depth % 128 == 0:
        gain_in, shift_in = gain.reshape(1, width), shift.reshape(1, width)
    else:
        gain_in, shift_in = (jnp.take(v, blocks, axis=0).reshape(1, width) for v in (gain, shift))
    out_bias = small[:, 2 * depth : 3 * depth].astype(F32) + small[:, 3 * depth : 4 * depth].astype(F32)
    cut = 4 * depth + qkv_bias.size
    bias_qkv = small[:, 4 * depth : cut].reshape(size, 3, heads, -1).transpose(1, 2, 0, 3).reshape(3, 1, inner)
    bias_fc1 = small[:, cut : cut + fc1_bias.size].reshape(size, heads, -1).transpose(1, 0, 2).reshape(1, hidden)
    dense_w = dense_w[0][:, :inner], dense_w[1][:, :inner], dense_w[2]
    dense_w, fc2_w = widen(dense_w, 2, wide), widen(fc2_w, 2, wide)
    qkv_w, fc1_w = widen(qkv_w, 2, wide), widen(fc1_w, 1, wide)

    tables = rotary_tables(LENGTH)
    normed, mean, inv_std = normalize(rows_all, gain_in, shift_in, enter, wide)
    qkv = project_qkv(normed, qkv_w)
    attn, query, key, value, lse = attention_forward(qkv, bias_qkv.astype(F32), tables)
    gelu, slope = project_fc1(normed, fc1_w, bias_fc1.astype(F32))
    branch = project_out(attn, gelu, dense_w, fc2_w)
    cot_all, _ = lax.optimization_barrier((cot_all, branch))
    branch = lax.psum_scatter(branch, "tensor", scatter_dimension=0, tiled=True)

    def columns(left, right):
        return lambda lo, hi: contract(left, right[:, lo * depth : hi * depth], ROWS)

    def rows(left, right):
        return lambda lo, hi: contract(left[:, lo * depth : hi * depth], right, ROWS)

    fc2_out = cube.scatter(columns(gelu, cot_all), down, 1)
    grad_pre, grad_fc1_bias = back_fc2(cot_all, fc2_w, slope)
    grad_attn = back_attn(cot_all, dense_w)
    *grads, grad_qkv_bias = attention_backward(query, key, value, attn, grad_attn, lse, tables)
    grad_rows, gain_part, shift_part = back_rows(
        grads, grad_pre, qkv_w, fc1_w, rows_all, mean, inv_std, enter
    )
    grad_rows, branch = lax.optimization_barrier((grad_rows, branch))
    grad_rows = lax.psum_scatter(grad_rows, "tensor", scatter_dimension=0, tiled=True)
    fc1_out = cube.scatter(rows(normed, grad_pre), up, 0)

    def qkv_columns(lo, hi):
        left = normed[:, lo * depth : hi * depth]
        return jnp.stack([contract(left, grad, ROWS) for grad in grads])

    qkv_out = cube.scatter(qkv_columns, down, 1)

    cot_part = jnp.sum(cotangent.astype(F32), axis=0).reshape(size, depth)
    sums = jnp.concatenate(
        [
            grad_qkv_bias.reshape(3, heads, size, -1).transpose(2, 0, 1, 3).reshape(size, -1),
            grad_fc1_bias.reshape(heads, size, -1).transpose(1, 0, 2).reshape(size, -1),
            cot_part,
        ],
        axis=1,
    )
    sums = jnp.concatenate(
        [gain_part.reshape(size, depth), shift_part.reshape(size, depth), jnp.take(sums, blocks, axis=0)], axis=1
    )
    count = sums.shape[1]
    extra = -(-count // depth // 16) * 16
    sums = jnp.pad(sums, ((0, 0), (0, extra * depth - count))).reshape(size, extra, depth)

    def dense_columns(lo, hi):
        part = contract(attn, cot_all[:, lo * depth : hi * depth], ROWS)
        return jnp.concatenate([part, sums[lo:hi].transpose(1, 0, 2).reshape(extra, -1)])

    dense_out = cube.scatter(dense_columns, up, 1)
    sums = dense_out[inner:].reshape(-1)
    dense_out = dense_out[:inner]
    ends = [depth, 2 * depth, 2 * depth + qkv_bias.size, 2 * depth + qkv_bias.size + fc1_bias.size, count]
    gain_out, shift_out, qkv_bias_out, fc1_bias_out, bias_out = jnp.split(sums[:count], ends[:-1])
    shared = jnp.concatenate([gain_out, shift_out, bias_out])
    ring = lax.axis_size("tensor")
    for bit in range(ring.bit_length() - 1):
        shared = shared + lax.ppermute(shared, "tensor", [(i, i ^ (1 << bit)) for i in range(ring)])
    gain_out, shift_out, bias_out = jnp.split(shared, 3)

    grad_rows, shared = lax.optimization_barrier((grad_rows, shared))
    if depth % 128:
        branch, grad_rows = (take_blocks(v, places, depth) for v in (branch, grad_rows))
    output = finish_output(tokens, branch, out_bias.reshape(1, width), leave, wide)
    grad_tokens = finish_tokens(tokens, cotangent, grad_rows, gain.reshape(1, width), leave, wide)
    return (
        output,
        grad_tokens,
        gain_out,
        shift_out,
        qkv_out.transpose(1, 0, 2),
        qkv_bias_out.reshape(qkv_bias.shape),
        dense_out,
        bias_out,
        fc1_out,
        fc1_bias_out.reshape(fc1_bias.shape),
        fc2_out,
        bias_out,
    )


def solution(mesh):
    in_specs = (
        P(("dp", "tensor"), None),
        P("dp"),
        P("dp"),
        P("dp", None, "tensor"),
        P(None, "tensor", "dp"),
        P("tensor", "dp"),
        P("dp"),
        P("dp", "tensor"),
        P("tensor", "dp"),
        P("tensor", "dp"),
        P("dp"),
        P(("dp", "tensor"), None),
    )
    out_specs = (
        P(("dp", "tensor"), None),
        P(("dp", "tensor"), None),
        P("dp"),
        P("dp"),
        P("dp", None, "tensor"),
        P(None, "tensor", "dp"),
        P("tensor", "dp"),
        P("dp"),
        P("dp", "tensor"),
        P("tensor", "dp"),
        P("tensor", "dp"),
        P("dp"),
    )
    step = functools.partial(body, mesh.shape["dp"])
    return jax.shard_map(step, mesh=mesh, in_specs=in_specs, out_specs=out_specs, check_vma=False)
```
